256 devices in a mesh: edge: 64 (over y, z, x_lo), chan: 4 (over x_hi, core).
Axes of the slice: x: 4 (x_hi: 2, x_lo: 2; x = x_hi * 2 + x_lo), y: 4, z: 8, core: 2. Of those that a mesh axis runs over, the one named last changes fastest.
Arguments:
- node_states: bfloat16 [1024, 49, 256], P('edge', None, 'chan'), may hold values from -6 to 6
- edge_vectors: float32 [3, 32768], P(None, ('edge', 'chan')), may hold values from -5.6 to 5.6, as said below
- source_part: int32 [32768, 1], P('edge'), may hold values from 0 to 63; in each aligned block of 512 rows (0 to 511, 512 to 1023, ...) at most 16 rows name the same one
- source_slot: int32 [32768], P('edge'), may hold values from 0 to 15
- target_slot: int32 [32768], P('edge'), may hold values from 0 to 15
- live_edges: int32 [64], P('edge'), may hold values from 1 to 512, 24576 in all
- weight_zero: bfloat16 [7, 256, 7, 256], P(None, 'chan'), may hold values from -0.125 to 0.125
- weight_one: bfloat16 [2, 6, 256, 6, 256], P(None, None, 'chan'), may hold values from -0.109375 to 0.109375
- weight_two: bfloat16 [2, 5, 256, 5, 256], P(None, None, 'chan'), may hold values from -0.125 to 0.125
Outputs:
- aggregated: bfloat16 [1024, 49, 256], P('edge', None, 'chan')
The draws below stay inside these ranges and needn't reach their ends.
Inputs may be any that keep to these rules, and one draw needn't show every extreme that they name: `source_part`: in each aligned block of 512 rows (the edges of one partition's slab) no partition number appears more than 16 times, and some number appears exactly 16 times. Edges are grouped by destination partition: the destination of an edge in slab p is node p * 16 + target_slot. `live_edges`: live slots stand at the front of each slab; the fullest slab is full. `edge_vectors`: every column has length between 0.8 and 5.6.
All inputs are finite; a program needn't handle non-finite values. No bound on the sum of `live_edges` on one device may be relied on, other than what follows from the above.
Results may differ from the reference program's by a relative error of at most 0.015.
Values may be sent and summed in bfloat16 or wider, within the bound.
No kernel may reach another device: no remote copies, remote signals or barrier semaphores. Data moves between devices by JAX's collectives and lax.ppermute only.
A program may use at most 128 MiB of HBM per device.

```python
import math
import jax
import jax.numpy as jnp
import numpy as np
from jax import lax

C = 256
LMAX = 6
MMAX = 2
N_DEV = 16
E_CAP = 512
NODES = 1024
EDGES = 32768
CAP = 16
COEFS = 49
KEPT = 29
N_EDGE = 64
N_CHAN = 4


def draw_edge_vectors(key, part):
    first_key, second_key = jax.random.split(jax.random.fold_in(key, 17))
    raw = jax.random.normal(first_key, (3, EDGES), jnp.float32)
    length = jax.random.uniform(second_key, (1, EDGES), jnp.float32, 0.8, 5.6)
    norm_value = jnp.sqrt(jnp.sum(raw * raw, axis=0, keepdims=True))
    direction = raw / jnp.maximum(norm_value, 1e-06)
    return jnp.clip(direction * length, -5.6, 5.6)


def with_ends(entries, rng, smallest, largest):
    index_at = [jax.random.randint(jax.random.fold_in(rng, axis), (), 0, length) for axis, length in enumerate(entries.shape)]
    longest = entries.shape.index(max(entries.shape))
    beside = index_at[:longest] + [(index_at[longest] + 1) % entries.shape[longest]] + index_at[longest + 1:]
    return entries.at[tuple(index_at)].set(smallest).at[tuple(beside)].set(largest)


def level_of(stream_key, shape, cuts, smallest, high):
    gain = 1.0
    for dim, shards_of in cuts:
        draws = jax.random.uniform(jax.random.fold_in(jax.random.fold_in(stream_key, 6), dim), (shards_of,), jnp.float32, smallest / len(cuts), high / len(cuts))
        gain = gain * jnp.repeat(jnp.exp(draws), shape[dim] // shards_of).reshape((-1,) + (1,) * (len(shape) - 1 - dim))
    return gain


def length_profile(number_of, total, bound, skew):
    portions = [(1 << 20) // math.isqrt(rank ** skew) + 1 for rank in range(2, number_of + 1)]
    spare, given = total - bound - (number_of - 1), [1] * (number_of - 1)
    while spare > 0:
        movable = [i for i in range(number_of - 1) if given[i] < bound]
        mass, budget = sum([portions[i] for i in movable]), spare
        for i in movable:
            more = min(bound - given[i], max(1, budget * portions[i] // mass), spare)
            given[i] = given[i] + more
            spare = spare - more
    return np.array([bound] + given)


def uneven_parts(stream_key, count, total, limit, lean):
    if count == 2:
        one = jax.random.randint(stream_key, (), max(1, total - limit), min(limit, total - 1) + 1)
        return jnp.stack([one, total - one])
    lengths = jnp.asarray(length_profile(count, total, limit, lean), jnp.int32)
    twos = (count - 1) // 2
    source_of, receiver = lengths[1:1 + 2 * twos:2], lengths[2:2 + 2 * twos:2]
    slack = jnp.minimum(source_of - 1, limit - receiver)
    passed = jax.random.randint(jax.random.fold_in(stream_key, 1), (twos,), 0, 1 << 20) % (slack + 1)
    lengths = lengths.at[1:1 + 2 * twos:2].set(source_of - passed).at[2:2 + 2 * twos:2].set(receiver + passed)
    return lengths[jax.random.permutation(jax.random.fold_in(stream_key, 2), count)]


def assign_block(own_key, own, number, rows, amount, top, most, lean):
    sequence = jax.random.permutation(own_key, amount)
    packed, usual = load_shares(amount, rows * top, most, lean, True), load_shares(amount, rows * top, most, lean, False)
    places = jnp.arange(amount)

    def named(sizes, turn):
        used = int((sizes > 0).sum())
        fixed = max(1, used // 4)
        passed = fixed + (places - fixed + turn * (used - fixed)) % max(1, amount - fixed)
        return jnp.zeros((amount,), jnp.int32).at[sequence[jnp.where(places < fixed, places, passed)]].set(jnp.asarray(sizes, jnp.int32))

    sizes = jnp.where(number % 4 == 0, named(packed, number // 4), named(usual, number - number // 4 - 1))
    mixed = jax.random.permutation(jax.random.fold_in(own, 3), amount)
    giver, receiver = mixed[0:amount // 2 * 2:2], mixed[1:amount // 2 * 2:2]
    room = jnp.minimum(sizes[giver] - 1, most - sizes[receiver]) // 2
    room = jnp.where((giver == sequence[0]) | (receiver == sequence[0]) | (sizes[receiver] == 0), 0, jnp.maximum(room, 0))
    passed = jax.random.randint(jax.random.fold_in(own, 4), (amount // 2,), 0, 1 << 20) % (room + 1)
    sizes = sizes.at[giver].add(-passed).at[receiver].add(passed)
    labels = jnp.searchsorted(jnp.cumsum(sizes), jnp.arange(rows * top), side="right").astype(jnp.int32)
    table = labels.reshape(top, rows).T
    table = table[jax.random.permutation(jax.random.fold_in(own, 1), rows)]
    turn = jax.random.randint(jax.random.fold_in(own, 2), (rows, 1), 0, top)
    return jnp.take_along_axis(table, (jnp.arange(top)[None, :] + turn) % top, axis=1)


def load_shares(count, total, bound, lean, full):
    loads = [(1 << 20) // math.isqrt(grade ** lean) + 1 for grade in range(1, count + 1)]
    largest = bound if full else min(bound, max(-(-total // count), total * loads[0] // sum(loads)))
    least = 1 if total - largest >= count - 1 else 0
    counts, rest = [largest] + [least] * (count - 1), total - largest - least * (count - 1)
    while rest > 0:
        movable = [i for i in range(1, count) if counts[i] < largest] or [i for i in range(1, count) if counts[i] < bound]
        mass, budget = sum([loads[i] for i in movable]), rest
        for i in movable:
            addition = min(bound - counts[i], max(1, budget * loads[i] // mass), rest)
            counts[i] = counts[i] + addition
            rest = rest - addition
    return np.array(counts)


def scatter_about(stream_key, shape, width, bound, cuts=(), kind=jnp.bfloat16):
    result = width * jax.random.normal(stream_key, shape, jnp.float32)
    if cuts:
        result = result * level_of(stream_key, shape, cuts, -0.22, 0.18)
    return jnp.clip(result, -bound, bound).astype(kind)


def setup_inputs(seed: int = 0) -> dict:
    splits = jax.random.split(jax.random.key(seed), 10)
    node_states = scatter_about(splits[0], (NODES, COEFS, C), 1.0, 6.0, ((0, 64), (2, 4)))
    edge_vectors = draw_edge_vectors(jax.random.fold_in(splits[9], 71), 0)
    source_part_keys = jax.random.split(jax.random.fold_in(splits[2], 1), EDGES // E_CAP)
    source_part_turns = jax.random.permutation(jax.random.fold_in(splits[2], 3), EDGES // E_CAP)
    source_part = jax.vmap(lambda own, number: assign_block(jax.random.fold_in(splits[2], 2), own, number, E_CAP, N_EDGE, 1, CAP, 2))(source_part_keys, source_part_turns).reshape((EDGES, 1))
    source_slot = with_ends(jax.random.randint(splits[3], (EDGES,), 0, N_DEV), jax.random.fold_in(splits[3], 1), 0, N_DEV - 1).astype(jnp.int32)
    target_slot = with_ends(jax.random.randint(splits[4], (EDGES,), 0, N_DEV), jax.random.fold_in(splits[4], 1), 0, N_DEV - 1).astype(jnp.int32)
    live_edges = uneven_parts(splits[5], N_EDGE, (3 * E_CAP * N_EDGE) // 4, E_CAP, 2).astype(jnp.int32)
    weight_zero = scatter_about(splits[6], (LMAX + 1, C, LMAX + 1, C), ((LMAX + 1) * C) ** -0.5, 0.125, ((1, 4),))
    weight_one = scatter_about(splits[7], (2, LMAX, C, LMAX, C), (2 * LMAX * C) ** -0.5, 0.109375, ((2, 4),))
    weight_two = scatter_about(splits[8], (2, LMAX - 1, C, LMAX - 1, C), (2 * (LMAX - 1) * C) ** -0.5, 0.125, ((2, 4),))
    return {"node_states": node_states, "edge_vectors": edge_vectors, "source_part": source_part, "source_slot": source_slot, "target_slot": target_slot, "live_edges": live_edges, "weight_zero": weight_zero, "weight_one": weight_one, "weight_two": weight_two}


cutoff_radius = 6.0
highest = lax.Precision.HIGHEST

def harmonics(coord_x, coord_y, coord_z, degree_top, order_top):
    results = {}
    real_part = [coord_x * 0.0 + 1.0]
    imag_part = [coord_x * 0.0]
    for azimuthal in range(1, order_top + 1):
        new_real = coord_x * real_part[-1] - coord_y * imag_part[-1]
        new_imag = coord_x * imag_part[-1] + coord_y * real_part[-1]
        real_part.append(new_real)
        imag_part.append(new_imag)
    for azimuthal in range(order_top + 1):
        start_value = (-1.0) ** azimuthal * math.prod(range(2 * azimuthal - 1, 0, -2))
        legendre = {azimuthal: coord_z * 0.0 + start_value}
        if azimuthal + 1 <= degree_top:
            legendre[azimuthal + 1] = coord_z * ((2 * azimuthal + 1) * start_value)
        for degree in range(azimuthal + 2, degree_top + 1):
            legendre[degree] = ((2 * degree - 1) * coord_z * legendre[degree - 1] - (degree + azimuthal - 1) * legendre[degree - 2]) / (degree - azimuthal)
        for degree in range(azimuthal, degree_top + 1):
            factor = math.sqrt((2 * degree + 1) / (4.0 * math.pi) * math.factorial(degree - azimuthal) / math.factorial(degree + azimuthal))
            if azimuthal == 0:
                results[degree, 0] = factor * legendre[degree]
            else:
                results[degree, azimuthal] = math.sqrt(2.0) * factor * legendre[degree] * real_part[azimuthal]
                results[degree, -azimuthal] = math.sqrt(2.0) * factor * legendre[degree] * imag_part[azimuthal]
    return results

def kept_rows():
    row_list = [(degree, 0) for degree in range(LMAX + 1)]
    for azimuthal in range(1, MMAX + 1):
        row_list += [(degree, azimuthal) for degree in range(azimuthal, LMAX + 1)]
        row_list += [(degree, -azimuthal) for degree in range(azimuthal, LMAX + 1)]
    return row_list

def invert_small(matrix):
    order_size = matrix.shape[0]
    work = np.concatenate([matrix, np.eye(order_size)], axis=1)
    for column in range(order_size):
        work[column] = work[column] / work[column, column]
        for row_index in range(order_size):
            if row_index != column:
                work[row_index] = work[row_index] - work[row_index, column] * work[column]
    return work[:, order_size:]

def sample_tables():
    sample_count = 2 * (LMAX + 1) ** 2
    positions = np.arange(sample_count) + 0.5
    height = 1.0 - 2.0 * positions / sample_count
    radius = np.sqrt(1.0 - height * height)
    azimuth = math.pi * (3.0 - math.sqrt(5.0)) * positions
    points = np.stack([radius * np.cos(azimuth), radius * np.sin(azimuth), height])
    values = harmonics(points[0], points[1], points[2], LMAX, LMAX)
    inverses = []
    for degree in range(LMAX + 1):
        sampled = np.stack([values[degree, azimuthal] for azimuthal in range(-degree, degree + 1)])
        inverses.append(sampled.T @ invert_small(sampled @ sampled.T))
    return (points, inverses)

def wigner_rows(vectors):
    length = jnp.sqrt(lax.optimization_barrier(jnp.sum(vectors * vectors, axis=0)))
    direction = vectors / length
    pick_first = jnp.where(jnp.abs(direction[0]) < 0.6, 1.0, 0.0).astype(jnp.float32)
    helper = jnp.stack([pick_first, 1.0 - pick_first, jnp.zeros_like(pick_first)])
    first_axis = jnp.cross(direction, helper, axis=0)
    first_axis = first_axis / jnp.sqrt(lax.optimization_barrier(jnp.sum(first_axis * first_axis, axis=0)))
    second_axis = jnp.cross(direction, first_axis, axis=0)
    frames = jnp.stack([first_axis, second_axis, direction])
    points, inverses = sample_tables()
    sample = jnp.asarray(points, jnp.float32)
    turned = jnp.einsum('rce,ck->rek', frames, sample, precision=highest)
    values = harmonics(turned[0], turned[1], turned[2], LMAX, MMAX)
    pieces = []
    for degree, azimuthal in kept_rows():
        table = jnp.asarray(inverses[degree], jnp.float32)
        pieces.append(jnp.dot(values[degree, azimuthal], table, precision=highest))
    compact = jnp.concatenate(pieces, axis=1)
    envelope = 0.5 * (jnp.cos(math.pi * length / cutoff_radius) + 1.0)
    return (compact, envelope)

def expand_rows(compact):
    padded_rows = []
    offset = 0
    for degree, azimuthal in kept_rows():
        span_size = 2 * degree + 1
        segment = compact[:, offset:offset + span_size]
        padded_rows.append(jnp.pad(segment, ((0, 0), (degree * degree, (LMAX + 1) ** 2 - degree * degree - span_size))))
        offset += span_size
    return jnp.stack(padded_rows, axis=1)

def convolve(turned, weight_zero, weight_one, weight_two, contract):
    end_zero = LMAX + 1
    end_one_plus = end_zero + LMAX
    end_one_minus = end_one_plus + LMAX
    end_two_plus = end_one_minus + LMAX - 1
    zero_part = turned[:end_zero]
    one_plus = turned[end_zero:end_one_plus]
    one_minus = turned[end_one_plus:end_one_minus]
    two_plus = turned[end_one_minus:end_two_plus]
    two_minus = turned[end_two_plus:]
    pattern = 'lce,lcjd->dje'
    out_zero = contract(pattern, zero_part, weight_zero)
    out_one_plus = contract(pattern, one_plus, weight_one[0]) - contract(pattern, one_minus, weight_one[1])
    out_one_minus = contract(pattern, one_minus, weight_one[0]) + contract(pattern, one_plus, weight_one[1])
    out_two_plus = contract(pattern, two_plus, weight_two[0]) - contract(pattern, two_minus, weight_two[1])
    out_two_minus = contract(pattern, two_minus, weight_two[0]) + contract(pattern, two_plus, weight_two[1])
    return jnp.concatenate([out_zero, out_one_plus, out_one_minus, out_two_plus, out_two_minus], axis=1)

def rounded(values):
    return lax.optimization_barrier(values.astype(jnp.bfloat16))

def float_contract(pattern, first_operand, second_operand):
    return jnp.einsum(pattern, first_operand.astype(jnp.float32), second_operand.astype(jnp.float32))

def reference(node_states, edge_vectors, source_part, source_slot, target_slot, live_edges, weight_zero, weight_one, weight_two):
    per_group = C // N_CHAN

    def one_slab(partition):
        first_edge = (partition * E_CAP).astype(jnp.int32)
        vectors = lax.dynamic_slice_in_dim(edge_vectors, first_edge, E_CAP, 1)
        compact, envelope = wigner_rows(vectors)
        rotation = expand_rows(rounded(compact))
        owner_part = lax.dynamic_slice_in_dim(source_part[:, 0], first_edge, E_CAP, 0)
        source_slots = lax.dynamic_slice_in_dim(source_slot, first_edge, E_CAP, 0)
        targets = lax.dynamic_slice_in_dim(target_slot, first_edge, E_CAP, 0)
        sources = node_states[owner_part * N_DEV + source_slots]
        turned = rounded(jnp.einsum('eik,ekc->ice', rotation.astype(jnp.float32), sources.astype(jnp.float32)))
        channel_mix = jnp.zeros((C, KEPT, E_CAP), jnp.float32)
        for group_index in range(N_CHAN):
            low_channel = group_index * per_group
            high_channel = low_channel + per_group
            partial_value = convolve(turned[:, low_channel:high_channel], weight_zero[:, low_channel:high_channel], weight_one[:, :, low_channel:high_channel], weight_two[:, :, low_channel:high_channel], float_contract)
            channel_mix = channel_mix + rounded(partial_value).astype(jnp.float32)
        alive_mask = (jnp.arange(E_CAP, dtype=jnp.int32) < live_edges[partition]).astype(jnp.float32)
        scaling = rounded(envelope).astype(jnp.float32) * alive_mask
        scaled = rounded(channel_mix * scaling)
        message = rounded(jnp.einsum('eik,cie->ekc', rotation.astype(jnp.float32), scaled.astype(jnp.float32)))
        selector = (jnp.arange(N_DEV, dtype=jnp.int32)[:, None] == targets[None, :]).astype(jnp.bfloat16)
        summed = jnp.dot(selector, message.reshape(E_CAP, COEFS * C), preferred_element_type=jnp.float32)
        return summed.astype(jnp.bfloat16).reshape(N_DEV, COEFS, C)
    blocks = lax.map(one_slab, jnp.arange(N_EDGE, dtype=jnp.int32))
    return blocks.reshape(NODES, COEFS, C)
```

```python
import math

import jax
import jax.numpy as jnp
import numpy as np
from jax import lax
from jax.sharding import Mesh
from jax.sharding import PartitionSpec as P

LMAX = 6
MMAX = 2
EDGE_AXES = ("y", "z", "xl")
CHAN_AXES = ("xh", "core")


cutoff_radius = 6.0
highest = lax.Precision.HIGHEST


def harmonics(coord_x, coord_y, coord_z, degree_top, order_top):
    results = {}
    real_part = [coord_x * 0.0 + 1.0]
    imag_part = [coord_x * 0.0]
    for azimuthal in range(1, order_top + 1):
        new_real = coord_x * real_part[-1] - coord_y * imag_part[-1]
        new_imag = coord_x * imag_part[-1] + coord_y * real_part[-1]
        real_part.append(new_real)
        imag_part.append(new_imag)
    for azimuthal in range(order_top + 1):
        start_value = (-1.0) ** azimuthal * math.prod(range(2 * azimuthal - 1, 0, -2))
        legendre = {azimuthal: coord_z * 0.0 + start_value}
        if azimuthal + 1 <= degree_top:
            legendre[azimuthal + 1] = coord_z * ((2 * azimuthal + 1) * start_value)
        for degree in range(azimuthal + 2, degree_top + 1):
            legendre[degree] = (
                (2 * degree - 1) * coord_z * legendre[degree - 1]
                - (degree + azimuthal - 1) * legendre[degree - 2]
            ) / (degree - azimuthal)
        for degree in range(azimuthal, degree_top + 1):
            factor = math.sqrt(
                (2 * degree + 1)
                / (4.0 * math.pi)
                * math.factorial(degree - azimuthal)
                / math.factorial(degree + azimuthal)
            )
            if azimuthal == 0:
                results[degree, 0] = factor * legendre[degree]
            else:
                results[degree, azimuthal] = (
                    math.sqrt(2.0) * factor * legendre[degree] * real_part[azimuthal]
                )
                results[degree, -azimuthal] = (
                    math.sqrt(2.0) * factor * legendre[degree] * imag_part[azimuthal]
                )
    return results


def kept_rows():
    row_list = [(degree, 0) for degree in range(LMAX + 1)]
    for azimuthal in range(1, MMAX + 1):
        row_list += [(degree, azimuthal) for degree in range(azimuthal, LMAX + 1)]
        row_list += [(degree, -azimuthal) for degree in range(azimuthal, LMAX + 1)]
    return row_list


def row_offsets():
    listing = []
    offset = 0
    for degree, azimuthal in kept_rows():
        listing.append((degree, offset))
        offset += 2 * degree + 1
    return listing


def invert_small(matrix):
    order_size = matrix.shape[0]
    work = np.concatenate([matrix, np.eye(order_size)], axis=1)
    for column in range(order_size):
        work[column] = work[column] / work[column, column]
        for row_index in range(order_size):
            if row_index != column:
                work[row_index] = work[row_index] - work[row_index, column] * work[column]
    return work[:, order_size:]


def sample_tables():
    sample_count = 2 * (LMAX + 1) ** 2
    positions = np.arange(sample_count) + 0.5
    height = 1.0 - 2.0 * positions / sample_count
    radius = np.sqrt(1.0 - height * height)
    azimuth = math.pi * (3.0 - math.sqrt(5.0)) * positions
    points = np.stack([radius * np.cos(azimuth), radius * np.sin(azimuth), height])
    values = harmonics(points[0], points[1], points[2], LMAX, LMAX)
    inverses = []
    for degree in range(LMAX + 1):
        sampled = np.stack([values[degree, azimuthal] for azimuthal in range(-degree, degree + 1)])
        inverses.append(sampled.T @ invert_small(sampled @ sampled.T))
    return (points, inverses)


def wigner_rows(vectors):
    length = jnp.sqrt(jnp.sum(vectors * vectors, axis=0))
    direction = vectors / length
    pick_first = jnp.where(jnp.abs(direction[0]) < 0.6, 1.0, 0.0).astype(jnp.float32)
    helper = jnp.stack([pick_first, 1.0 - pick_first, jnp.zeros_like(pick_first)])
    first_axis = jnp.cross(direction, helper, axis=0)
    first_axis = first_axis / jnp.sqrt(jnp.sum(first_axis * first_axis, axis=0))
    second_axis = jnp.cross(direction, first_axis, axis=0)
    frames = jnp.stack([first_axis, second_axis, direction])
    points, inverses = sample_tables()
    sample = jnp.asarray(points, jnp.float32)
    turned = jnp.einsum("rce,ck->rek", frames, sample, precision=highest)
    values = harmonics(turned[0], turned[1], turned[2], LMAX, MMAX)
    pieces = []
    for degree, azimuthal in kept_rows():
        table = jnp.asarray(inverses[degree], jnp.float32)
        pieces.append(jnp.dot(values[degree, azimuthal], table, precision=highest))
    compact = jnp.concatenate(pieces, axis=1)
    envelope = 0.5 * (jnp.cos(math.pi * length / cutoff_radius) + 1.0)
    return (compact, envelope)


def rotate_forward(compact_t, sources):
    rows_out = []
    for degree, offset in row_offsets():
        total = compact_t[offset].astype(jnp.float32)[None, :] * sources[degree * degree].astype(
            jnp.float32
        )
        for inner in range(1, 2 * degree + 1):
            total = total + compact_t[offset + inner].astype(jnp.float32)[None, :] * sources[
                degree * degree + inner
            ].astype(jnp.float32)
        rows_out.append(total)
    return jnp.stack(rows_out, axis=0).astype(jnp.bfloat16)


def convolve(turned, weight_zero, weight_one, weight_two, contract):
    end_zero = LMAX + 1
    end_one_plus = end_zero + LMAX
    end_one_minus = end_one_plus + LMAX
    end_two_plus = end_one_minus + LMAX - 1
    zero_part = turned[:end_zero]
    one_plus = turned[end_zero:end_one_plus]
    one_minus = turned[end_one_plus:end_one_minus]
    two_plus = turned[end_one_minus:end_two_plus]
    two_minus = turned[end_two_plus:]
    pattern = "lce,lcjd->jed"
    out_zero = contract(pattern, zero_part, weight_zero)
    out_one_plus = contract(pattern, one_plus, weight_one[0]) - contract(
        pattern, one_minus, weight_one[1]
    )
    out_one_minus = contract(pattern, one_minus, weight_one[0]) + contract(
        pattern, one_plus, weight_one[1]
    )
    out_two_plus = contract(pattern, two_plus, weight_two[0]) - contract(
        pattern, two_minus, weight_two[1]
    )
    out_two_minus = contract(pattern, two_minus, weight_two[0]) + contract(
        pattern, two_plus, weight_two[1]
    )
    return jnp.concatenate(
        [out_zero, out_one_plus, out_one_minus, out_two_plus, out_two_minus], axis=0
    )


def mixed_contract(pattern, first_operand, second_operand):
    return jnp.einsum(pattern, first_operand, second_operand, preferred_element_type=jnp.float32)


def one_hot(indices, width):
    return (indices[:, None] == jnp.arange(width, dtype=jnp.int32)[None, :]).astype(jnp.bfloat16)


def shards(
    node_states,
    edge_vectors,
    source_part,
    source_slot,
    target_slot,
    live_edges,
    weight_zero,
    weight_one,
    weight_two,
):
    slab_size = source_slot.shape[0]
    local_nodes = node_states.shape[0]
    local_channels = node_states.shape[2]
    coef_count = node_states.shape[1]
    group_count = lax.axis_size(EDGE_AXES)
    node_flat = node_states.reshape(local_nodes, coef_count * local_channels)
    pair = lax.all_gather(node_flat, "xl", axis=0, tiled=True)
    table = lax.all_gather(pair, ("y", "z"), axis=0, tiled=True)
    vectors = lax.all_gather(edge_vectors, CHAN_AXES, axis=1, tiled=True)
    compact, envelope = wigner_rows(vectors)
    compact_t = compact.astype(jnp.bfloat16).T
    source_index = source_part[:, 0] * local_nodes + source_slot
    selector = one_hot(source_index, group_count * local_nodes)
    sources = (
        lax.dot_general(
            table, selector, (((0,), (1,)), ((), ())), preferred_element_type=jnp.float32
        )
        .astype(jnp.bfloat16)
        .reshape(coef_count, local_channels, slab_size)
    )
    turned = rotate_forward(compact_t, sources)
    mixed = convolve(turned, weight_zero, weight_one, weight_two, mixed_contract).astype(
        jnp.bfloat16
    )
    alive_mask = (jnp.arange(slab_size, dtype=jnp.int32) < live_edges[0]).astype(jnp.float32)
    scaling = envelope * alive_mask
    targets = jnp.where(
        jnp.arange(local_nodes, dtype=jnp.int32)[:, None] == target_slot[None, :],
        scaling[None, :],
        0.0,
    )
    partial_out = []
    listing = row_offsets()
    for degree in range(LMAX + 1):
        rows = [(r, o) for r, (d, o) in enumerate(listing) if d == degree]
        left = jnp.stack(
            [
                targets[None, :, :] * compact_t[o : o + 2 * degree + 1].astype(jnp.float32)[:, None, :]
                for _, o in rows
            ]
        ).astype(jnp.bfloat16)
        right = jnp.stack([mixed[r] for r, _ in rows])
        partial_out.append(
            jnp.einsum("rkte,red->tkd", left, right, preferred_element_type=jnp.float32)
        )
    partial_sum = jnp.concatenate(partial_out, axis=1).astype(jnp.bfloat16)
    return lax.psum_scatter(partial_sum, CHAN_AXES, scatter_dimension=2, tiled=True)


def solution(mesh):
    in_specs = (
        P(EDGE_AXES, None, CHAN_AXES),
        P(None, EDGE_AXES + CHAN_AXES),
        P(EDGE_AXES, None),
        P(EDGE_AXES),
        P(EDGE_AXES),
        P(EDGE_AXES),
        P(None, CHAN_AXES, None, None),
        P(None, None, CHAN_AXES, None, None),
        P(None, None, CHAN_AXES, None, None),
    )
    out_specs = P(EDGE_AXES, None, CHAN_AXES)
    fine = Mesh(mesh.devices.reshape(4, 8, 2, 2, 2), EDGE_AXES + CHAN_AXES)
    return jax.shard_map(shards, mesh=fine, in_specs=in_specs, out_specs=out_specs, check_vma=False)
```

```python
import math

import jax
import jax.numpy as jnp
import numpy as np
from jax import lax
from jax.experimental import pallas as pl
from jax.experimental.pallas import tpu as pltpu
from jax.sharding import Mesh
from jax.sharding import PartitionSpec as P

LMAX = 6
MMAX = 2
EDGE_AXES = ("y", "z", "xl")
CHAN_AXES = ("xh", "core")
SIZE_Y, SIZE_Z, SIZE_XL, SIZE_XH, SIZE_CORE = 4, 8, 2, 2, 2
LANES = 128
COEFS = (LMAX + 1) ** 2

cutoff_radius = 6.0


def solid_harmonics(x, y, z, r2, degree_top, order_top):
    results = {}
    real_part = [x * 0.0 + 1.0]
    imag_part = [x * 0.0]
    for _ in range(order_top):
        new_real = x * real_part[-1] - y * imag_part[-1]
        new_imag = x * imag_part[-1] + y * real_part[-1]
        real_part.append(new_real)
        imag_part.append(new_imag)
    for m in range(order_top + 1):
        start = (-1.0) ** m * math.prod(range(2 * m - 1, 0, -2))
        legendre = {m: z * 0.0 + start}
        if m + 1 <= degree_top:
            legendre[m + 1] = z * ((2 * m + 1) * start)
        for l in range(m + 2, degree_top + 1):
            legendre[l] = z * legendre[l - 1] * ((2 * l - 1) / (l - m)) - r2 * legendre[l - 2] * (
                (l + m - 1) / (l - m)
            )
        for l in range(m, degree_top + 1):
            factor = harmonic_norm(l, m)
            if m == 0:
                results[l, 0] = factor * legendre[l]
            else:
                results[l, m] = math.sqrt(2.0) * factor * (legendre[l] * real_part[m])
                results[l, -m] = math.sqrt(2.0) * factor * (legendre[l] * imag_part[m])
    return results


def harmonic_norm(l, m):
    return math.sqrt(
        (2 * l + 1) / (4.0 * math.pi) * math.factorial(l - m) / math.factorial(l + m)
    )


def gradient_tables():
    count = 60
    steps = np.arange(count) + 0.5
    points = np.stack([np.cos(steps * 1.7), np.sin(steps * 2.3), np.cos(steps * 0.9 + 0.4)])
    base = solid_harmonics(*points, (points**2).sum(0), LMAX, LMAX)
    tables = {}
    for axis in range(3):
        moved = points.astype(np.complex128)
        moved[axis] += 1e-20j
        value = solid_harmonics(*moved, (moved**2).sum(0), LMAX, LMAX)
        for l in range(1, LMAX + 1):
            lower = np.stack([base[l - 1, m] for m in range(-l + 1, l)], axis=1)
            for m in range(-l, l + 1):
                fit = np.linalg.lstsq(lower, value[l, m].imag / 1e-20, rcond=None)[0]
                tables[l, axis, m] = [
                    (i - l + 1, float(g)) for i, g in enumerate(fit) if abs(g) > 1e-8
                ]
    return tables


def kept_rows():
    row_list = [(degree, 0) for degree in range(LMAX + 1)]
    for azimuthal in range(1, MMAX + 1):
        row_list += [(degree, azimuthal) for degree in range(azimuthal, LMAX + 1)]
        row_list += [(degree, -azimuthal) for degree in range(azimuthal, LMAX + 1)]
    return row_list


def row_offsets():
    listing = []
    offset = 0
    for degree, _ in kept_rows():
        listing.append((degree, offset))
        offset += 2 * degree + 1
    return listing


ROWS = kept_rows()
OFFSETS = row_offsets()
ROT_TOTAL = sum(2 * degree + 1 for degree, _ in ROWS)
DEGREE_ROWS = {
    degree: [i for i, (d, _) in enumerate(ROWS) if d == degree] for degree in range(LMAX + 1)
}
MIX_PLACE = {}
for _degree in range(LMAX + 1):
    for _row in DEGREE_ROWS[_degree]:
        MIX_PLACE[_row] = len(MIX_PLACE)
SECTIONS = ((0, 7, 0), (7, 6, 256), (13, 6, 512), (19, 5, 768), (24, 5, 1024))


def frame_kernel(place_ref, info_ref, rot_ref, edge_ref, index_ref):
    vx, vy, vz = info_ref[0], info_ref[1], info_ref[2]
    length = jnp.sqrt(vx * vx + vy * vy + vz * vz)
    ux, uy, uz = vx / length, vy / length, vz / length
    first = jnp.where(jnp.abs(ux) < 0.6, 1.0, 0.0)
    second = 1.0 - first
    ax, ay, az = -uz * second, uz * first, ux * second - uy * first
    norm = jnp.sqrt(ax * ax + ay * ay + az * az)
    ax, ay, az = ax / norm, ay / norm, az / norm
    bx, by, bz = uy * az - uz * ay, uz * ax - ux * az, ux * ay - uy * ax
    values = solid_harmonics(ux, uy, uz, 1.0, LMAX, LMAX)
    tables = gradient_tables()

    def along(direction, lower, l):
        products = {}
        out = {}
        for m in range(-l, l + 1):
            total = None
            for axis in range(3):
                for lower_m, g in tables[l, axis, m]:
                    if lower_m not in lower:
                        continue
                    key = (axis, lower_m)
                    if key not in products:
                        products[key] = direction[axis] * lower[lower_m]
                    term = products[key] * g
                    total = term if total is None else total + term
            out[m] = total
        return out

    a, b = (ax, ay, az), (bx, by, bz)
    grad_a, grad_b = {}, {}
    where = {(d, m): off for (d, m), (_, off) in zip(ROWS, OFFSETS)}

    def put(l, m, rows, factor):
        for i, k in enumerate(range(-l, l + 1)):
            rot_ref[where[l, m] + i] = rows[k] * factor

    for l in range(LMAX + 1):
        here = {m: values[l, m] for m in range(-l, l + 1)}
        put(l, 0, here, math.sqrt(4.0 * math.pi / (2 * l + 1)))
        if l >= 1:
            lower = {m: values[l - 1, m] for m in range(-l + 1, l)}
            grad_a[l] = along(a, lower, l)
            grad_b[l] = along(b, lower, l)
            k1 = math.sqrt(2.0) * harmonic_norm(l, 1) * (-l * (l + 1) / 2)
            put(l, 1, grad_a[l], 1.0 / k1)
            put(l, -1, grad_b[l], 1.0 / k1)
        if l >= 2:
            k2 = math.sqrt(2.0) * harmonic_norm(l, 2) * ((l + 2) * (l + 1) * l * (l - 1) / 8)
            aa = along(a, grad_a[l - 1], l)
            bb = along(b, grad_b[l - 1], l)
            ab = along(a, grad_b[l - 1], l)
            put(l, 2, {k: aa[k] - bb[k] for k in aa}, 1.0 / (4 * k2))
            put(l, -2, ab, 1.0 / (2 * k2))
    envelope = 0.5 * (jnp.cos(math.pi / cutoff_radius * length) + 1.0)
    edge_ref[0] = envelope * info_ref[5]
    edge_ref[1] = info_ref[4]
    source = info_ref[3].astype(jnp.int32)
    part = source >> 4
    far_y = (part >> 4) ^ place_ref[0]
    far_z = (place_ref[1] - ((part >> 1) & 7)) & 7
    far_x = (part & 1) ^ place_ref[2]
    index_ref[...] = (
        ((((far_y >> 1) * 8 + far_z) * 2 + (far_y & 1)) * 2 + far_x) * 16 + (source & 15)
    )


def edge_frames(info, place):
    return pl.pallas_call(
        frame_kernel,
        out_shape=(
            jax.ShapeDtypeStruct((ROT_TOTAL, 8, LANES), jnp.float32),
            jax.ShapeDtypeStruct((2, 8, LANES), jnp.float32),
            jax.ShapeDtypeStruct((8, LANES), jnp.int32),
        ),
        in_specs=[
            pl.BlockSpec(memory_space=pltpu.SMEM),
            pl.BlockSpec(memory_space=pltpu.VMEM),
        ],
        out_specs=(pl.BlockSpec(memory_space=pltpu.VMEM),) * 3,
        name="edge_frames",
    )(place, info)


def layer_kernel(
    rot_ref,
    edge_ref,
    index_ref,
    w0_ref,
    w1_ref,
    w2_ref,
    *rest,
    nodes,
    width,
    blocks,
):
    block_refs = rest[:blocks]
    out0_ref, out1_ref = rest[blocks : blocks + 2]
    table, hot, source, turned, mix, left, sems = rest[blocks + 2 :]
    rows = nodes // blocks
    copies = [
        pltpu.make_async_copy(
            block_refs[i], table.at[pl.ds(i * rows, rows)], sems.at[i]
        )
        for i in range(blocks)
    ]
    for copy in copies:
        copy.start()
    for g in range(8):
        number = lax.broadcasted_iota(jnp.int32, (nodes, LANES), 0)
        hot[:, g * LANES : (g + 1) * LANES] = jnp.where(
            number == index_ref[g : g + 1, :], 1.0, 0.0
        ).astype(jnp.bfloat16)
    for copy in copies:
        copy.wait()
    step = 4 * width
    total = COEFS * width
    for start in range(0, total, step):
        size = min(step, total - start)
        source[start : start + size, :] = lax.dot_general(
            table[:, start : start + size],
            hot[...],
            (((0,), (0,)), ((), ())),
            preferred_element_type=jnp.float32,
        )

    def turn(g, carry):
        lanes = pl.ds(pl.multiple_of(g * LANES, LANES), LANES)
        for first, count, base in SECTIONS:
            for n in range(count):
                degree, offset = OFFSETS[first + n]
                acc = None
                for k in range(2 * degree + 1):
                    at = (degree * degree + k) * width
                    term = rot_ref[offset + k, pl.ds(g, 1), :] * source[at : at + width, lanes]
                    acc = term if acc is None else acc + term
                turned[base + n * width : base + (n + 1) * width, lanes] = acc.astype(jnp.bfloat16)
        return carry

    lax.fori_loop(0, 8, turn, 0)

    half = 4 * LANES

    def slab(s, carry):
        cols = pl.ds(pl.multiple_of(s * half, half), half)

        def section(n):
            _, count, base = SECTIONS[n]
            return turned[base : base + count * width, cols]

        def apply(part, weight):
            return lax.dot_general(
                part, weight, (((0,), (0,)), ((), ())), preferred_element_type=jnp.float32
            )

        def keep(row, value):
            at = MIX_PLACE[row] * half
            mix[at : at + half, :] = value.astype(jnp.bfloat16)

        zero = section(0)
        for j in range(7):
            keep(j, apply(zero, w0_ref[:, j * 256 : (j + 1) * 256]))
        for weight, plus_at, minus_at in ((w1_ref, 1, 2), (w2_ref, 3, 4)):
            plus, minus = section(plus_at), section(minus_at)
            for j in range(SECTIONS[plus_at][1]):
                real = weight[0, :, j * 256 : (j + 1) * 256]
                imag = weight[1, :, j * 256 : (j + 1) * 256]
                keep(SECTIONS[plus_at][0] + j, apply(plus, real) - apply(minus, imag))
                keep(SECTIONS[minus_at][0] + j, apply(minus, real) + apply(plus, imag))
        slots = lax.broadcasted_iota(jnp.int32, (16, LANES), 0).astype(jnp.float32)
        masks = [
            jnp.where(
                slots == edge_ref[1, pl.ds(s * 4 + g, 1), :],
                edge_ref[0, pl.ds(s * 4 + g, 1), :],
                0.0,
            )
            for g in range(4)
        ]
        for degree in range(LMAX + 1):
            members = DEGREE_ROWS[degree]
            for place, row in enumerate(members):
                offset = OFFSETS[row][1]
                for k in range(2 * degree + 1):
                    for g in range(4):
                        at = place * half + g * LANES
                        left[k * 16 : (k + 1) * 16, at : at + LANES] = (
                            masks[g] * rot_ref[offset + k, pl.ds(s * 4 + g, 1), :]
                        ).astype(jnp.bfloat16)
            depth = len(members) * half
            first = MIX_PLACE[members[0]] * half
            height = (2 * degree + 1) * 16
            result = jnp.dot(
                left[:height, :depth],
                mix[first : first + depth, :],
                preferred_element_type=jnp.float32,
            )
            at = pl.ds(pl.multiple_of(s * (COEFS * 16) + degree * degree * 16, 16), height)
            out0_ref[at, :] = jnp.concatenate(
                [result[:, 0:64], result[:, 128:192]], axis=1
            ).astype(jnp.bfloat16)
            out1_ref[at, :] = jnp.concatenate(
                [result[:, 64:128], result[:, 192:256]], axis=1
            ).astype(jnp.bfloat16)
        return carry

    lax.fori_loop(0, 2, slab, 0)


def layer(rot, edge, index, w0, w1, w2, block_list):
    blocks = len(block_list)
    rows, features = block_list[0].shape
    nodes = blocks * rows
    width = features // COEFS
    vmem = pl.BlockSpec(memory_space=pltpu.VMEM)

    def body(*refs):
        layer_kernel(*refs, nodes=nodes, width=width, blocks=blocks)

    shape = jax.ShapeDtypeStruct((2 * COEFS * 16, LANES), jnp.bfloat16)
    return pl.pallas_call(
        body,
        out_shape=(shape, shape),
        in_specs=[vmem] * 6 + [pl.BlockSpec(memory_space=pl.ANY)] * blocks,
        out_specs=(vmem, vmem),
        scratch_shapes=[
            pltpu.VMEM((nodes, features), jnp.bfloat16),
            pltpu.VMEM((nodes, 8 * LANES), jnp.bfloat16),
            pltpu.VMEM((features, 8 * LANES), jnp.float32),
            pltpu.VMEM((1280, 8 * LANES), jnp.bfloat16),
            pltpu.VMEM((len(ROWS) * 4 * LANES, 256), jnp.bfloat16),
            pltpu.VMEM((208, 5 * 4 * LANES), jnp.bfloat16),
            pltpu.SemaphoreType.DMA((blocks,)),
        ],
        compiler_params=pltpu.CompilerParams(vmem_limit_bytes=60 * 1024 * 1024),
        name="layer",
    )(rot, edge, index, w0, w1, w2, *block_list)


def move(block, flip_y=0, shift_z=0, flip_x=0):
    pairs = []
    for y in range(SIZE_Y):
        for z in range(SIZE_Z):
            for x in range(SIZE_XL):
                pairs.append(
                    (
                        (y * SIZE_Z + z) * SIZE_XL + x,
                        ((y ^ flip_y) * SIZE_Z + (z + shift_z) % SIZE_Z) * SIZE_XL + (x ^ flip_x),
                    )
                )
    return lax.ppermute(block, EDGE_AXES, pairs)


def gather_blocks(own, other):
    near = jnp.concatenate(
        [own, move(other, flip_x=1), move(own, flip_y=1), move(other, flip_y=1, flip_x=1)], axis=0
    )
    far = move(near, flip_y=2)
    first, second = {0: near}, {0: far}
    for s in range(1, 4):
        for ring in (first, second):
            ring[s] = move(ring[s - 1], shift_z=1)
            ring[8 - s] = move(ring[(9 - s) % 8], shift_z=-1)
    first[4] = move(first[3], shift_z=1)
    second[4] = move(second[5], shift_z=-1)
    return [first[s] for s in range(8)] + [second[s] for s in range(8)]


def shards(
    node_states,
    edge_vectors,
    source_part,
    source_slot,
    target_slot,
    live_edges,
    weight_zero,
    weight_one,
    weight_two,
):
    local_nodes, coef_count, local_channels = node_states.shape
    half_channels = local_channels // 2
    quarter = edge_vectors.shape[1]
    at_y, at_z, at_x = lax.axis_index("y"), lax.axis_index("z"), lax.axis_index("xl")
    at_h, at_c = lax.axis_index("xh"), lax.axis_index("core")
    begin = (at_h * SIZE_CORE + at_c) * quarter

    def mine(array):
        return lax.dynamic_slice_in_dim(array, begin, quarter, 0)

    source = mine(source_part[:, 0]) * local_nodes + mine(source_slot)
    alive = (begin + jnp.arange(quarter, dtype=jnp.int32)) < live_edges[0]
    info = jnp.concatenate(
        [
            edge_vectors,
            jnp.stack(
                [
                    source.astype(jnp.float32),
                    mine(target_slot).astype(jnp.float32),
                    alive.astype(jnp.float32),
                ]
            ),
        ],
        axis=0,
    )
    info = lax.all_gather(info, ("xl", "xh", "core"), axis=1)
    place = jnp.stack([at_y, at_z, at_x]).astype(jnp.int32)
    rot, edge, index = edge_frames(info, place)

    halves = node_states.reshape(local_nodes, coef_count, 2, half_channels)
    own = lax.dynamic_index_in_dim(halves, at_x, 2, keepdims=False)
    other = lax.dynamic_index_in_dim(halves, 1 - at_x, 2, keepdims=False)
    features = coef_count * half_channels
    block_list = gather_blocks(
        own.reshape(local_nodes, features), other.reshape(local_nodes, features)
    )

    low = at_x * half_channels
    w0 = lax.dynamic_slice_in_dim(weight_zero, low, half_channels, 1).reshape(
        7 * half_channels, 7 * 256
    )
    w1 = lax.dynamic_slice_in_dim(weight_one, low, half_channels, 2).reshape(
        2, 6 * half_channels, 6 * 256
    )
    w2 = lax.dynamic_slice_in_dim(weight_two, low, half_channels, 2).reshape(
        2, 5 * half_channels, 5 * 256
    )
    part0, part1 = layer(rot, edge, index, w0, w1, w2, block_list)

    swap = [(0, 1), (1, 0)]
    kept = jnp.where(at_c == 0, part0, part1)
    sent = jnp.where(at_c == 0, part1, part0)
    summed = kept.astype(jnp.float32) + lax.ppermute(sent, "core", swap).astype(jnp.float32)
    rows = coef_count * local_nodes
    summed = summed.reshape(2, rows, LANES)
    to_send = lax.dynamic_index_in_dim(summed, 1 - at_x, 0, keepdims=False).astype(jnp.bfloat16)
    summed = lax.dynamic_index_in_dim(summed, at_x, 0, keepdims=False)
    summed = summed + lax.ppermute(to_send, "xl", swap).astype(jnp.float32)

    def packed(value):
        return jnp.concatenate([value[: rows // 2], value[rows // 2 :]], axis=1)

    low_part, high_part = packed(summed[:, :64]), packed(summed[:, 64:])
    to_send = jnp.where(at_h == 0, high_part, low_part).astype(jnp.bfloat16)
    stay = jnp.where(at_h == 0, low_part, high_part)
    stay = stay + lax.ppermute(to_send, "xh", swap).astype(jnp.float32)
    stay = stay.astype(jnp.bfloat16)
    stay = jnp.concatenate([stay[:, :64], stay[:, 64:]], axis=0)
    return stay.reshape(coef_count, local_nodes, local_channels).transpose(1, 0, 2)


def solution(mesh):
    in_specs = (
        P(EDGE_AXES, None, CHAN_AXES),
        P(None, EDGE_AXES + CHAN_AXES),
        P(EDGE_AXES, None),
        P(EDGE_AXES),
        P(EDGE_AXES),
        P(EDGE_AXES),
        P(None, CHAN_AXES, None, None),
        P(None, None, CHAN_AXES, None, None),
        P(None, None, CHAN_AXES, None, None),
    )
    out_specs = P(EDGE_AXES, None, CHAN_AXES)
    fine = Mesh(
        mesh.devices.reshape(SIZE_Y, SIZE_Z, SIZE_XL, SIZE_XH, SIZE_CORE), EDGE_AXES + CHAN_AXES
    )
    return jax.shard_map(
        shards, mesh=fine, in_specs=in_specs, out_specs=out_specs, check_vma=False
    )
```
